32 devices in a mesh: dp: 4 (over x, core), half: 2 (over y), own: 4 (over z).
Axes of the slice: x: 2, y: 2, z: 4, core: 2. Of those that a mesh axis runs over, the one named last changes fastest.
Arguments:
- grad_parts: bfloat16 [4, 6, 1024, 1024], P('dp', None, ('half', 'own')), may hold values from -6 to 6
- owner_table: int32 [6, 1], replicated, may hold values from 0 to 3; in each aligned block of 6 rows (0 to 5, 6 to 11, ...) at most 2 rows name the same one
- left_basis: bfloat16 [8, 1024, 1024], P(('half', 'own')), may hold values from -0.1875 to 0.1875
- right_basis: bfloat16 [8, 1024, 1024], P(('half', 'own')), may hold values from -0.1875 to 0.1875
- first_moment: bfloat16 [8, 1024, 1024], P(('half', 'own'), 'dp'), may hold values from -6 to 6
- second_moment: bfloat16 [8, 1024, 1024], P(('half', 'own'), 'dp'), may hold values from 0.5 to 8
Outputs:
- update: bfloat16 [6, 1024, 1024], P(None, ('half', 'own'), 'dp')
The draws below stay inside these ranges and needn't reach their ends.
Inputs may be any that keep to these rules, and one draw needn't show every extreme that they name: `owner_table`: every owner index is named by at least one block and by at most 2 blocks; some owner is named by exactly 2 blocks.
All inputs are finite; a program needn't handle non-finite values.
Results may differ from the reference program's by a relative error of at most 0.013.
Values may be sent and summed in bfloat16 or wider, within the bound.
A program may use at most 128 MiB of HBM per device.

```python
import math
import jax
import jax.numpy as jnp
import numpy as np
from jax import lax

B = 1024
BLOCKS = 6
SLOTS = 8
N_DP = 4
N_HALF = 2
N_OWN = 4


def block_scale(rng, extent, shards, least, largest):
    def one(axis_at, parts):
        draws = jax.random.uniform(jax.random.fold_in(jax.random.fold_in(rng, 6), axis_at), (parts,), jnp.float32, least / len(shards), largest / len(shards))
        return jnp.repeat(jnp.exp(draws), extent[axis_at] // parts).reshape((-1,) + (1,) * (len(extent) - axis_at - 1))

    factor_of = one(*shards[0])
    for cut in shards[1:]:
        factor_of = factor_of * one(*cut)
    return factor_of


def shared_out(rng, own, number, rows, amount, top, limit, slope):
    sequence = jax.random.permutation(rng, amount)
    heavy_load, ordinary = shares(amount, rows * top, limit, slope, True), shares(amount, rows * top, limit, slope, False)
    places = jnp.arange(amount)

    def named(sizes, offset_by):
        used = int((sizes > 0).sum())
        fixed = max(1, used // 4)
        passed = fixed + (places - fixed + offset_by * (used - fixed)) % max(1, amount - fixed)
        return jnp.zeros((amount,), jnp.int32).at[sequence[jnp.where(places < fixed, places, passed)]].set(jnp.asarray(sizes, jnp.int32))

    sizes = jnp.where(number % 4 == 0, named(heavy_load, number // 4), named(ordinary, number - number // 4 - 1))
    mixed = jax.random.permutation(jax.random.fold_in(own, 3), amount)
    donor, sink = mixed[0:amount // 2 * 2:2], mixed[1:amount // 2 * 2:2]
    margin = jnp.minimum(sizes[donor] - 1, limit - sizes[sink]) // 2
    margin = jnp.where((donor == sequence[0]) | (sink == sequence[0]) | (sizes[sink] == 0), 0, jnp.maximum(margin, 0))
    passed = jax.random.randint(jax.random.fold_in(own, 4), (amount // 2,), 0, 1 << 20) % (margin + 1)
    sizes = sizes.at[donor].add(-passed).at[sink].add(passed)
    items = jnp.searchsorted(jnp.cumsum(sizes), jnp.arange(rows * top), side="right").astype(jnp.int32)
    grid = items.reshape(top, rows).T
    grid = grid[jax.random.permutation(jax.random.fold_in(own, 1), rows)]
    offset_by = jax.random.randint(jax.random.fold_in(own, 2), (rows, 1), 0, top)
    return jnp.take_along_axis(grid, (jnp.arange(top)[None, :] + offset_by) % top, axis=1)


def shares(count, total, reach, lean, full):
    portions = [(1 << 20) // math.isqrt(grade ** lean) + 1 for grade in range(1, count + 1)]
    largest = reach if full else min(reach, max(-(-total // count), total * portions[0] // sum(portions)))
    least = 1 if total - largest >= count - 1 else 0
    holding, surplus = [largest] + [least] * (count - 1), total - largest - least * (count - 1)
    while surplus > 0:
        candidates = [i for i in range(1, count) if holding[i] < largest] or [i for i in range(1, count) if holding[i] < reach]
        pool, budget = sum([portions[i] for i in candidates]), surplus
        for i in candidates:
            extra = min(reach - holding[i], max(1, budget * portions[i] // pool), surplus)
            holding[i] = holding[i] + extra
            surplus = surplus - extra
    return np.array(holding)


def centred(rng, extent, spread, limit, pieces=(), kind=jnp.bfloat16):
    values = jax.random.normal(rng, extent, jnp.float32) * spread
    if len(pieces) > 0:
        values = block_scale(rng, extent, pieces, -0.22, 0.18) * values
    return jnp.clip(values, min=-limit, max=limit).astype(kind)


def setup_inputs(seed: int = 0) -> dict:
    arg_keys = jax.random.split(jax.random.key(seed), 7)
    grad_parts = centred(arg_keys[0], (N_DP, BLOCKS, B, B), 1.0, 6.0, ((0, 4), (2, 8)))
    owner_table_keys = jax.random.split(jax.random.fold_in(arg_keys[1], 1), BLOCKS // BLOCKS)
    owner_table_turns = jax.random.permutation(jax.random.fold_in(arg_keys[1], 3), BLOCKS // BLOCKS)
    owner_table = jax.vmap(lambda own, number: shared_out(jax.random.fold_in(arg_keys[1], 2), own, number, BLOCKS, N_OWN, 1, N_HALF, 2))(owner_table_keys, owner_table_turns).reshape((BLOCKS, 1))
    left_basis = centred(arg_keys[2], (SLOTS, B, B), B ** -0.5, 0.1875, ((0, 8),))
    right_basis = centred(arg_keys[3], (SLOTS, B, B), B ** -0.5, 0.1875, ((0, 8),))
    first_moment = centred(arg_keys[4], (SLOTS, B, B), 1.0, 6.0, ((0, 8), (1, 4)))
    second_moment = jnp.clip(jnp.exp(math.log(8.0) - 2.7725887 * jax.random.uniform(arg_keys[5], (SLOTS, B, B), jnp.float32) ** block_scale(arg_keys[5], (SLOTS, B, B), ((0, 8), (1, 4)), -0.2, 0.2)), 0.5, 8.0).astype(jnp.bfloat16)
    return dict(grad_parts=grad_parts, owner_table=owner_table, left_basis=left_basis, right_basis=right_basis, first_moment=first_moment, second_moment=second_moment)


beta_first = 0.9
beta_second = 0.95
bias_first = 1.0 - 0.9 ** 10
bias_second = 1.0 - 0.95 ** 10
epsilon = 1e-08

def slot_numbers(owner_table):
    owner_ids = owner_table[:, 0].astype(jnp.int32)
    positions = jnp.arange(owner_ids.shape[0], dtype=jnp.int32)
    shared = (owner_ids[:, None] == owner_ids[None, :]) & (positions[None, :] < positions[:, None])
    ranking = lax.optimization_barrier(jnp.sum(shared.astype(jnp.int32), axis=1)).astype(jnp.int32)
    return (ranking * N_OWN + owner_ids).astype(jnp.int32)

def reference(grad_parts, owner_table, left_basis, right_basis, first_moment, second_moment):
    running = grad_parts[0].astype(jnp.float32)
    for replica in range(1, N_DP):
        running = running + grad_parts[replica].astype(jnp.float32)
    gradient = running.astype(jnp.bfloat16)
    slot_ids = slot_numbers(owner_table)

    def per_block(inputs):
        block_grad, slot_index = inputs
        left_matrix = left_basis[slot_index]
        right_matrix = right_basis[slot_index]
        projected = jnp.dot(left_matrix.T, block_grad, preferred_element_type=jnp.float32).astype(jnp.bfloat16)
        rotated = jnp.dot(projected, right_matrix, preferred_element_type=jnp.float32)
        first_new = beta_first * first_moment[slot_index].astype(jnp.float32) + (1.0 - beta_first) * rotated
        second_new = beta_second * second_moment[slot_index].astype(jnp.float32) + (1.0 - beta_second) * rotated * rotated
        direction = (first_new / bias_first / (jnp.sqrt(second_new / bias_second) + epsilon)).astype(jnp.bfloat16)
        back = jnp.dot(direction, right_matrix.T, preferred_element_type=jnp.float32).astype(jnp.bfloat16)
        update = jnp.dot(left_matrix, back, preferred_element_type=jnp.float32)
        return update.astype(jnp.bfloat16)
    return lax.map(per_block, (gradient, slot_ids))
```

```python
import functools

import jax
import jax.numpy as jnp
from jax import lax
from jax.experimental import pallas as pl
from jax.experimental.pallas import tpu as pltpu
from jax.sharding import PartitionSpec as P

beta_first = 0.9
beta_second = 0.95
bias_first = 1.0 - 0.9**10
bias_second = 1.0 - 0.95**10
epsilon = 1e-08


def slot_select(owner_table, owner_count, slot_count):
    owner_ids = owner_table[:, 0]
    positions = jnp.arange(owner_ids.shape[0], dtype=jnp.int32)
    shared = (owner_ids[:, None] == owner_ids[None, :]) & (positions[None, :] < positions[:, None])
    ranking = jnp.sum(shared.astype(jnp.int32), axis=1)
    slot_ids = ranking * owner_count + owner_ids
    slot_range = jnp.arange(slot_count, dtype=jnp.int32)
    return (slot_range[:, None] == slot_ids[None, :]).astype(jnp.bfloat16)


def local(grad_parts, owner_table, left_basis, right_basis, first_moment, second_moment):
    halves = lax.axis_size("half")
    owners = lax.axis_size("own")
    replicas = lax.axis_size("dp")
    block_count = grad_parts.shape[1]
    piece_rows = grad_parts.shape[2]
    block_width = grad_parts.shape[3]
    quarter = block_width // replicas
    offset = lax.axis_index("dp") * quarter
    summed = lax.psum_scatter(
        grad_parts[0].astype(jnp.float32).astype(jnp.bfloat16),
        "dp",
        scatter_dimension=2,
        tiled=True,
    )
    selector = slot_select(owner_table, owners, halves * owners)
    flat_grad = summed.reshape(block_count, piece_rows * quarter)
    packed = jnp.dot(selector, flat_grad, preferred_element_type=jnp.float32).astype(jnp.bfloat16)
    packed = packed.reshape(halves, owners, piece_rows, quarter)
    arrived = lax.all_to_all(
        lax.all_to_all(packed, "half", split_axis=0, concat_axis=0, tiled=True),
        "own",
        split_axis=1,
        concat_axis=1,
        tiled=True,
    )
    grad_block = arrived.reshape(block_width, quarter)
    left_matrix = left_basis[0]
    right_matrix = right_basis[0]
    right_rows = lax.dynamic_slice_in_dim(right_matrix, offset, quarter, 0)
    left_slice = lax.dynamic_slice_in_dim(left_matrix, offset, quarter, 1)
    projected = lax.dot_general(
        left_slice,
        lax.all_gather(grad_block, "dp", axis=1, tiled=True),
        (((0,), (0,)), ((), ())),
        preferred_element_type=jnp.float32,
    )
    rotated = jnp.dot(
        projected.astype(jnp.bfloat16), right_matrix, preferred_element_type=jnp.float32
    )
    first_new = beta_first * first_moment[0].astype(jnp.float32) + (1.0 - beta_first) * rotated
    second_new = (
        beta_second * second_moment[0].astype(jnp.float32) + (1.0 - beta_second) * rotated * rotated
    )
    direction = (first_new / bias_first / (jnp.sqrt(second_new / bias_second) + epsilon)).astype(
        jnp.bfloat16
    )
    partial_cols = lax.dot_general(
        lax.all_gather(direction, "dp", axis=0, tiled=True),
        right_rows,
        (((1,), (1,)), ((), ())),
        preferred_element_type=jnp.float32,
    )
    update_block = jnp.dot(
        left_matrix, partial_cols.astype(jnp.bfloat16), preferred_element_type=jnp.float32
    )
    outgoing = update_block.astype(jnp.bfloat16).reshape(halves, owners, piece_rows, quarter)
    returned = lax.all_to_all(
        lax.all_to_all(outgoing, "half", split_axis=0, concat_axis=0, tiled=True),
        "own",
        split_axis=1,
        concat_axis=1,
        tiled=True,
    )
    flat_back = returned.reshape(halves * owners, piece_rows * quarter)
    placed = lax.dot_general(
        selector, flat_back, (((0,), (0,)), ((), ())), preferred_element_type=jnp.float32
    )
    return placed.astype(jnp.bfloat16).reshape(block_count, piece_rows, quarter)


MESH = pl.DeviceIdType.MESH
LANES = 128
TILE_ROWS = 16


def pick(index, values):
    chosen = values[0]
    for i in range(1, len(values)):
        chosen = lax.select_n(index == i, chosen, values[i])
    return chosen


def step_kernel(
    sizes,
    table,
    grad,
    left_in,
    right_in,
    first_in,
    second_in,
    out,
    left,
    right,
    first,
    second,
    own,
    near,
    paired,
    far_in,
    packed,
    grad_cols,
    grad_turned,
    proj_out,
    proj_in,
    proj,
    direction,
    back_out,
    back_in,
    update,
    returned,
    load_sem,
    own_sem,
    near_sem,
    far_sem,
    slot_sem,
    proj_sem,
    back_sem,
    return_sem,
):
    replicas, halves, owners, blocks, rows, width, chunks, subs = sizes
    far = replicas // 2
    group = halves * owners
    quarter = width // replicas
    cols = quarter // chunks
    sub_rows = rows // subs
    me_dp = lax.axis_index("dp")
    me_group = lax.axis_index("half") * owners + lax.axis_index("own")
    me_far = me_dp // 2
    parity = me_dp % 2
    mate = me_far * 2 + 1 - parity

    def dp_id(index):
        return {"dp": index}

    def group_id(index):
        return {"half": index // owners, "own": index % owners}

    def remote(src, dst, sems, index_out, index_in, target):
        return pltpu.make_async_remote_copy(
            src_ref=src,
            dst_ref=dst,
            send_sem=sems.at[(0,) + index_out],
            recv_sem=sems.at[(1,) + index_in],
            device_id=target,
            device_id_type=MESH,
        )

    def columns(quarter_index, chunk):
        return pl.ds(pl.multiple_of(quarter_index * quarter + chunk * cols, LANES), cols)

    pieces = [(k, r) for k in range(chunks) for r in range(subs)]
    order = list(range(1, far)) + [0]

    own_loads = {}
    for k, r in pieces:
        for j in order:
            index = ((me_far + j) % far) * 2 + parity
            own_loads[j, k, r] = pltpu.make_async_copy(
                grad.at[:, pl.ds(r * sub_rows, sub_rows), columns(index, k)],
                own[j][k][r],
                own_sem.at[j, k, r],
            )
            own_loads[j, k, r].start()

    barrier = pltpu.get_barrier_semaphore()
    for j in range(1, replicas):
        pl.semaphore_signal(
            barrier, inc=1, device_id=dp_id((me_dp + j) % replicas), device_id_type=MESH
        )
    for t in range(1, group):
        pl.semaphore_signal(
            barrier, inc=1, device_id=group_id((me_group + t) % group), device_id_type=MESH
        )
    pl.semaphore_wait(barrier, replicas - 1 + group - 1)

    sends = []
    back_own = {}

    near_copies = {}
    for k, r in pieces:
        for j in order:
            index = ((me_far + j) % far) * 2 + 1 - parity
            copy = remote(
                grad.at[:, pl.ds(r * sub_rows, sub_rows), columns(index, k)],
                near[j][k][r],
                near_sem,
                (j, k, r),
                (j, k, r),
                dp_id(mate),
            )
            copy.start()
            near_copies[j, k, r] = copy
            sends.append(copy)

    loads = [
        pltpu.make_async_copy(left_in.at[0], left, load_sem.at[0]),
        pltpu.make_async_copy(right_in.at[0], right, load_sem.at[1]),
        pltpu.make_async_copy(first_in.at[0], first, load_sem.at[2]),
        pltpu.make_async_copy(second_in.at[0], second, load_sem.at[3]),
    ]
    for load in loads:
        load.start()

    def slot_of(b):
        owner = table[b, 0]
        rank = lax.fori_loop(
            0, b, lambda c, n: n + jnp.where(table[c, 0] == owner, 1, 0), jnp.int32(0)
        )
        return rank * owners + owner

    slots = [slot_of(b) for b in range(blocks)]
    block_of = []
    for s in range(group):
        found = jnp.int32(0)
        for b in range(blocks):
            found = jnp.where(slots[b] == s, jnp.int32(b), found)
        block_of.append(found)

    far_copies = {}
    for k, r in pieces:
        for j in range(1, far):
            own_loads[j, k, r].wait()
            near_copies[j, k, r].wait_recv()
            for b in range(blocks):
                paired[j - 1][k][r][b] = (
                    own[j][k][r][b].astype(jnp.float32) + near[j][k][r][b].astype(jnp.float32)
                ).astype(jnp.bfloat16)
            copy = remote(
                paired[j - 1][k][r],
                far_in[j - 1][k][r],
                far_sem,
                (j - 1, k, r),
                (j - 1, k, r),
                dp_id(((me_far + j) % far) * 2 + parity),
            )
            copy.start()
            far_copies[j, k, r] = copy
            sends.append(copy)

    def pack(k, r):
        own_loads[0, k, r].wait()
        near_copies[0, k, r].wait_recv()
        for j in range(1, far):
            far_copies[j, k, r].wait_recv()
        gradients = []
        for b in range(blocks):
            total = own[0][k][r][b].astype(jnp.float32) + near[0][k][r][b].astype(jnp.float32)
            for j in range(1, far):
                total = total + far_in[j - 1][k][r][b].astype(jnp.float32)
            gradients.append(total.astype(jnp.bfloat16))
        for s in range(group):
            packed[k][r][s] = pick(block_of[s], gradients)
        here = pl.ds(pl.multiple_of(me_group * rows + r * sub_rows, TILE_ROWS), sub_rows)
        for t in range(1, group):
            to = (me_group + t) % group
            copy = remote(
                packed[k][r].at[to],
                grad_cols[k].at[here],
                slot_sem,
                (k, r, to),
                (k, r, me_group),
                group_id(to),
            )
            copy.start()
            sends.append(copy)

    def project(k):
        for r in range(subs):
            for t in range(1, group):
                source = (me_group + t) % group
                there = pl.ds(pl.multiple_of(source * rows + r * sub_rows, TILE_ROWS), sub_rows)
                remote(
                    packed[k][r].at[source],
                    grad_cols[k].at[there],
                    slot_sem,
                    (k, r, source),
                    (k, r, source),
                    group_id(source),
                ).wait_recv()
        for r in range(subs):
            here = pl.ds(pl.multiple_of(me_group * rows + r * sub_rows, TILE_ROWS), sub_rows)
            grad_cols[k][here] = packed[k][r][me_group]
        grad_turned[...] = grad_cols[k][...].T
        for e in range(replicas):
            proj_out[k][e] = jnp.dot(
                grad_turned[...],
                left[:, e * quarter : (e + 1) * quarter],
                preferred_element_type=jnp.float32,
            ).astype(jnp.bfloat16)
        for j in [*range(2, replicas), 1]:
            to = (me_dp + j) % replicas
            copy = remote(
                proj_out[k].at[to],
                proj_in[k].at[me_dp],
                proj_sem,
                (k, to),
                (k, me_dp),
                dp_id(to),
            )
            copy.start()
            sends.append(copy)

    def turn(k):
        for j in range(replicas):
            source = (me_dp + j) % replicas
            if j > 0:
                remote(
                    proj_out[k].at[source],
                    proj_in[k].at[source],
                    proj_sem,
                    (k, source),
                    (k, source),
                    dp_id(source),
                ).wait_recv()
        proj_in[k][me_dp] = proj_out[k][me_dp]
        for e in range(replicas):
            first_col = e * quarter + k * cols
            proj[:, first_col : first_col + cols] = proj_in[k][e].T

    for k, r in pieces:
        pack(k, r)
    for k in range(chunks):
        if k == 0:
            loads[0].wait()
        project(k)
    for k in range(chunks):
        turn(k)
    for load in loads[1:]:
        load.wait()

    for e in range(replicas):
        part = slice(e * quarter, (e + 1) * quarter)
        rotated = jnp.dot(proj[...], right[:, part], preferred_element_type=jnp.float32)
        first_new = beta_first * first[:, part].astype(jnp.float32) + (1.0 - beta_first) * rotated
        second_new = (
            beta_second * second[:, part].astype(jnp.float32)
            + (1.0 - beta_second) * rotated * rotated
        )
        direction[:, part] = (
            first_new / bias_first / (jnp.sqrt(second_new / bias_second) + epsilon)
        ).astype(jnp.bfloat16)

    for k in range(chunks):
        for j in [*range(2, replicas), 1, 0]:
            to = (me_dp + j) % replicas
            these = right[pl.ds(pl.multiple_of(to * quarter + k * cols, LANES), cols), :]
            result = lax.dot_general(
                direction[...], these, (((1,), (1,)), ((), ())), preferred_element_type=jnp.float32
            ).astype(jnp.bfloat16)
            if j == 0:
                back_own[k] = result
            else:
                back_out[k][j - 1][...] = result
                copy = remote(
                    back_out[k][j - 1],
                    back_in[k].at[me_dp],
                    back_sem,
                    (k, to),
                    (k, me_dp),
                    dp_id(to),
                )
                copy.start()
                sends.append(copy)

    for k in range(chunks):
        for j in range(1, replicas):
            source = (me_dp + j) % replicas
            remote(
                back_out[k][j - 1],
                back_in[k].at[source],
                back_sem,
                (k, source),
                (k, source),
                dp_id(source),
            ).wait_recv()
        back_in[k][me_dp] = back_own[k]
        update[k][...] = (
            jnp.dot(
                left[...], back_in[k][...].reshape(width, cols), preferred_element_type=jnp.float32
            )
            .astype(jnp.bfloat16)
            .reshape(group, rows, cols)
        )
        for t in range(1, group):
            to = (me_group + t) % group
            copy = remote(
                update[k].at[to],
                returned[k].at[me_group],
                return_sem,
                (k, to),
                (k, me_group),
                group_id(to),
            )
            copy.start()
            sends.append(copy)

    for k in range(chunks):
        for t in range(1, group):
            source = (me_group + t) % group
            remote(
                update[k].at[source],
                returned[k].at[source],
                return_sem,
                (k, source),
                (k, source),
                group_id(source),
            ).wait_recv()
        returned[k][me_group] = update[k][me_group]
        arrived = [returned[k][s] for s in range(group)]
        for b in range(blocks):
            out[b, :, k * cols : (k + 1) * cols] = pick(slots[b], arrived)

    for copy in sends:
        copy.wait_send()


def nest(counts, shape):
    if not counts:
        return pltpu.VMEM(shape, jnp.bfloat16)
    return [nest(counts[1:], shape) for _ in range(counts[0])]


def fused(grad_parts, owner_table, left_basis, right_basis, first_moment, second_moment):
    replicas, halves, owners = (lax.axis_size(a) for a in ("dp", "half", "own"))
    blocks, rows, width = grad_parts.shape[1:]
    quarter = width // replicas
    group = halves * owners
    far = replicas // 2
    chunks = quarter // LANES
    subs = 2 if rows % (2 * TILE_ROWS) == 0 else 1
    cols, sub_rows = quarter // chunks, rows // subs
    sizes = (replicas, halves, owners, blocks, rows, width, chunks, subs)
    bf16, dma = jnp.bfloat16, pltpu.SemaphoreType.DMA
    hbm = pl.BlockSpec(memory_space=pl.ANY)
    return pl.pallas_call(
        functools.partial(step_kernel, sizes),
        out_shape=jax.ShapeDtypeStruct((blocks, rows, quarter), bf16),
        in_specs=[pl.BlockSpec(memory_space=pltpu.SMEM)] + [hbm] * 5,
        out_specs=pl.BlockSpec(memory_space=pltpu.VMEM),
        scratch_shapes=[
            pltpu.VMEM((width, width), bf16),
            pltpu.VMEM((width, width), bf16),
            pltpu.VMEM((quarter, width), bf16),
            pltpu.VMEM((quarter, width), bf16),
            nest((far, chunks, subs), (blocks, sub_rows, cols)),
            nest((far, chunks, subs), (blocks, sub_rows, cols)),
            nest((far - 1, chunks, subs), (blocks, sub_rows, cols)),
            nest((far - 1, chunks, subs), (blocks, sub_rows, cols)),
            nest((chunks, subs), (group, sub_rows, cols)),
            nest((chunks,), (width, cols)),
            pltpu.VMEM((cols, width), bf16),
            nest((chunks,), (replicas, cols, quarter)),
            nest((chunks,), (replicas, cols, quarter)),
            pltpu.VMEM((quarter, width), bf16),
            pltpu.VMEM((quarter, width), bf16),
            nest((chunks, replicas - 1), (quarter, cols)),
            nest((chunks,), (replicas, quarter, cols)),
            nest((chunks,), (group, rows, cols)),
            nest((chunks,), (group, rows, cols)),
            dma((4,)),
            dma((far, chunks, subs)),
            dma((2, far, chunks, subs)),
            dma((2, far - 1, chunks, subs)),
            dma((2, chunks, subs, group)),
            dma((2, chunks, replicas)),
            dma((2, chunks, replicas)),
            dma((2, chunks, group)),
        ],
        compiler_params=pltpu.CompilerParams(collective_id=0, has_side_effects=True),
    )(owner_table, grad_parts.reshape(blocks, rows, width), left_basis, right_basis, first_moment, second_moment)


def fits_kernel(mesh, rows, width):
    replicas = mesh.shape["dp"]
    return (
        replicas >= 4
        and replicas % 2 == 0
        and rows % TILE_ROWS == 0
        and width % (replicas * LANES) == 0
    )


def route(mesh, *arrays):
    rows = arrays[0].shape[2]
    body = fused if fits_kernel(mesh, rows, arrays[0].shape[3]) else local
    return body(*arrays)


def solution(mesh):
    return jax.shard_map(
        functools.partial(route, mesh),
        mesh=mesh,
        in_specs=(
            P("dp", None, ("half", "own"), None),
            P(),
            P(("half", "own"), None, None),
            P(("half", "own"), None, None),
            P(("half", "own"), "dp", None),
            P(("half", "own"), "dp", None),
        ),
        out_specs=P(None, ("half", "own"), "dp"),
        check_vma=False,
    )
```

```python
import functools
import math

import jax
import jax.numpy as jnp
from jax import lax
from jax.experimental import pallas as pl
from jax.experimental.pallas import tpu as pltpu
from jax.sharding import PartitionSpec as P

beta_first = 0.9
beta_second = 0.95
bias_first = 1.0 - 0.9**10
bias_second = 1.0 - 0.95**10
epsilon = 1e-08


def slot_select(owner_table, owner_count, slot_count):
    owner_ids = owner_table[:, 0]
    positions = jnp.arange(owner_ids.shape[0], dtype=jnp.int32)
    shared = (owner_ids[:, None] == owner_ids[None, :]) & (positions[None, :] < positions[:, None])
    ranking = jnp.sum(shared.astype(jnp.int32), axis=1)
    slot_ids = ranking * owner_count + owner_ids
    slot_range = jnp.arange(slot_count, dtype=jnp.int32)
    return (slot_range[:, None] == slot_ids[None, :]).astype(jnp.bfloat16)


def local(grad_parts, owner_table, left_basis, right_basis, first_moment, second_moment):
    halves = lax.axis_size("half")
    owners = lax.axis_size("own")
    replicas = lax.axis_size("dp")
    block_count = grad_parts.shape[1]
    piece_rows = grad_parts.shape[2]
    block_width = grad_parts.shape[3]
    quarter = block_width // replicas
    offset = lax.axis_index("dp") * quarter
    summed = lax.psum_scatter(
        grad_parts[0].astype(jnp.float32).astype(jnp.bfloat16),
        "dp",
        scatter_dimension=2,
        tiled=True,
    )
    selector = slot_select(owner_table, owners, halves * owners)
    flat_grad = summed.reshape(block_count, piece_rows * quarter)
    packed = jnp.dot(selector, flat_grad, preferred_element_type=jnp.float32).astype(jnp.bfloat16)
    packed = packed.reshape(halves, owners, piece_rows, quarter)
    arrived = lax.all_to_all(
        lax.all_to_all(packed, "half", split_axis=0, concat_axis=0, tiled=True),
        "own",
        split_axis=1,
        concat_axis=1,
        tiled=True,
    )
    grad_block = arrived.reshape(block_width, quarter)
    left_matrix = left_basis[0]
    right_matrix = right_basis[0]
    right_rows = lax.dynamic_slice_in_dim(right_matrix, offset, quarter, 0)
    left_slice = lax.dynamic_slice_in_dim(left_matrix, offset, quarter, 1)
    projected = lax.dot_general(
        left_slice,
        lax.all_gather(grad_block, "dp", axis=1, tiled=True),
        (((0,), (0,)), ((), ())),
        preferred_element_type=jnp.float32,
    )
    rotated = jnp.dot(
        projected.astype(jnp.bfloat16), right_matrix, preferred_element_type=jnp.float32
    )
    first_new = beta_first * first_moment[0].astype(jnp.float32) + (1.0 - beta_first) * rotated
    second_new = (
        beta_second * second_moment[0].astype(jnp.float32) + (1.0 - beta_second) * rotated * rotated
    )
    direction = (first_new / bias_first / (jnp.sqrt(second_new / bias_second) + epsilon)).astype(
        jnp.bfloat16
    )
    partial_cols = lax.dot_general(
        lax.all_gather(direction, "dp", axis=0, tiled=True),
        right_rows,
        (((1,), (1,)), ((), ())),
        preferred_element_type=jnp.float32,
    )
    update_block = jnp.dot(
        left_matrix, partial_cols.astype(jnp.bfloat16), preferred_element_type=jnp.float32
    )
    outgoing = update_block.astype(jnp.bfloat16).reshape(halves, owners, piece_rows, quarter)
    returned = lax.all_to_all(
        lax.all_to_all(outgoing, "half", split_axis=0, concat_axis=0, tiled=True),
        "own",
        split_axis=1,
        concat_axis=1,
        tiled=True,
    )
    flat_back = returned.reshape(halves * owners, piece_rows * quarter)
    placed = lax.dot_general(
        selector, flat_back, (((0,), (0,)), ((), ())), preferred_element_type=jnp.float32
    )
    return placed.astype(jnp.bfloat16).reshape(block_count, piece_rows, quarter)


MESH = pl.DeviceIdType.MESH
LANES = 128
TILE_ROWS = 16


def pick(index, values):
    chosen = values[0]
    for i in range(1, len(values)):
        chosen = lax.select_n(index == i, chosen, values[i])
    return chosen


def step_kernel(
    sizes,
    table,
    grad,
    left_in,
    right_in,
    first_in,
    second_in,
    out,
    left,
    right,
    first,
    second,
    own,
    lent,
    near,
    paired,
    far_in,
    packed,
    grad_cols,
    grad_turned,
    proj_out,
    proj_in,
    proj,
    partial,
    direction,
    back_out,
    back_in,
    update,
    returned,
    load_sem,
    right_sem,
    own_sem,
    lent_sem,
    near_sem,
    far_sem,
    slot_sem,
    proj_sem,
    back_sem,
    return_sem,
):
    replicas, halves, owners, blocks, rows, width, chunks, subs = sizes
    far = replicas // 2
    group = halves * owners
    quarter = width // replicas
    cols = quarter // chunks
    sub_rows = rows // subs
    me_dp = lax.axis_index("dp")
    me_group = lax.axis_index("half") * owners + lax.axis_index("own")
    me_far = me_dp // 2
    parity = me_dp % 2
    mate = me_far * 2 + 1 - parity

    middle = max(1, owners // 2)
    me_half, me_own = me_group // owners, me_group % owners
    side = me_own // middle
    others = []
    for across in range(owners // middle - 1, -1, -1):
        for i in range(middle):
            for h in range(halves):
                if across or i or h:
                    o = (side + across) % (owners // middle) * middle + (me_own + i) % middle
                    others.append((me_half + h) % halves * owners + o)

    def dp_id(index):
        return {"dp": index}

    def group_id(index):
        return {"half": index // owners, "own": index % owners}

    def remote(src, dst, sems, index_out, index_in, target):
        return pltpu.make_async_remote_copy(
            src_ref=src,
            dst_ref=dst,
            send_sem=sems.at[(0,) + index_out],
            recv_sem=sems.at[(1,) + index_in],
            device_id=target,
            device_id_type=MESH,
        )

    def columns(quarter_index, chunk):
        return pl.ds(pl.multiple_of(quarter_index * quarter + chunk * cols, LANES), cols)

    pieces = [(k, r) for k in range(chunks) for r in range(subs)]
    order = list(range(1, far)) + [0]

    own_loads, lent_loads = {}, {}
    for k, r in pieces:
        for j in order:
            for side, into, sems, copies in (
                (1 - parity, lent, lent_sem, lent_loads),
                (parity, own, own_sem, own_loads),
            ):
                index = ((me_far + j) % far) * 2 + side
                copies[j, k, r] = pltpu.make_async_copy(
                    grad.at[:, pl.ds(r * sub_rows, sub_rows), columns(index, k)],
                    into[j][k][r],
                    sems.at[j, k, r],
                )
                copies[j, k, r].start()

    barrier = pltpu.get_barrier_semaphore()
    for j in range(1, replicas):
        pl.semaphore_signal(
            barrier, inc=1, device_id=dp_id((me_dp + j) % replicas), device_id_type=MESH
        )
    for t in range(1, group):
        pl.semaphore_signal(
            barrier, inc=1, device_id=group_id((me_group + t) % group), device_id_type=MESH
        )
    pl.semaphore_wait(barrier, replicas - 1 + group - 1)

    sends = []
    back_own = {}

    near_copies = {}
    for k, r in pieces:
        for j in order:
            lent_loads[j, k, r].wait()
            copy = remote(
                lent[j][k][r],
                near[j][k][r],
                near_sem,
                (j, k, r),
                (j, k, r),
                dp_id(mate),
            )
            copy.start()
            near_copies[j, k, r] = copy
            sends.append(copy)

    loads = [
        pltpu.make_async_copy(left_in.at[0], left, load_sem.at[0]),
        pltpu.make_async_copy(first_in.at[0], first, load_sem.at[1]),
        pltpu.make_async_copy(second_in.at[0], second, load_sem.at[2]),
    ]
    for load in loads:
        load.start()
    right_loads = [
        pltpu.make_async_copy(
            right_in.at[0, pl.ds(e * quarter + k * cols, cols)],
            right[k].at[pl.ds(e * cols, cols)],
            right_sem.at[k, e],
        )
        for k in range(chunks)
        for e in range(replicas)
    ]
    for load in right_loads:
        load.start()

    def slot_of(b):
        owner = table[b]
        rank = lax.fori_loop(
            0, b, lambda c, n: n + jnp.where(table[c] == owner, 1, 0), jnp.int32(0)
        )
        return rank * owners + owner

    slots = [slot_of(b) for b in range(blocks)]
    block_of = []
    for s in range(group):
        found = jnp.int32(0)
        for b in range(blocks):
            found = jnp.where(slots[b] == s, jnp.int32(b), found)
        block_of.append(found)

    far_copies = {}
    for k, r in pieces:
        for j in range(1, far):
            own_loads[j, k, r].wait()
            near_copies[j, k, r].wait_recv()
            for b in range(blocks):
                paired[j - 1][k][r][b] = (
                    own[j][k][r][b].astype(jnp.float32) + near[j][k][r][b].astype(jnp.float32)
                ).astype(jnp.bfloat16)
            copy = remote(
                paired[j - 1][k][r],
                far_in[j - 1][k][r],
                far_sem,
                (j - 1, k, r),
                (j - 1, k, r),
                dp_id(((me_far + j) % far) * 2 + parity),
            )
            copy.start()
            far_copies[j, k, r] = copy
            sends.append(copy)

    def pack(k, r):
        own_loads[0, k, r].wait()
        near_copies[0, k, r].wait_recv()
        for j in range(1, far):
            far_copies[j, k, r].wait_recv()
        gradients = []
        for b in range(blocks):
            total = own[0][k][r][b].astype(jnp.float32) + near[0][k][r][b].astype(jnp.float32)
            for j in range(1, far):
                total = total + far_in[j - 1][k][r][b].astype(jnp.float32)
            gradients.append(total.astype(jnp.bfloat16))
        for s in range(group):
            packed[k][r][s] = pick(block_of[s], gradients)
        here = pl.ds(pl.multiple_of(me_group * rows + r * sub_rows, TILE_ROWS), sub_rows)
        for to in others:
            copy = remote(
                packed[k][r].at[to],
                grad_cols[k].at[here],
                slot_sem,
                (k, r, to),
                (k, r, me_group),
                group_id(to),
            )
            copy.start()
            sends.append(copy)

    def project(k):
        for r in range(subs):
            for source in others:
                there = pl.ds(pl.multiple_of(source * rows + r * sub_rows, TILE_ROWS), sub_rows)
                remote(
                    packed[k][r].at[source],
                    grad_cols[k].at[there],
                    slot_sem,
                    (k, r, source),
                    (k, r, source),
                    group_id(source),
                ).wait_recv()
        for r in range(subs):
            here = pl.ds(pl.multiple_of(me_group * rows + r * sub_rows, TILE_ROWS), sub_rows)
            grad_cols[k][here] = packed[k][r][me_group]
        grad_turned[...] = grad_cols[k][...].T
        for e in range(replicas):
            proj_out[k][e] = jnp.dot(
                grad_turned[...],
                left[:, e * quarter : (e + 1) * quarter],
                preferred_element_type=jnp.float32,
            ).astype(jnp.bfloat16)
        for j in [*range(2, replicas), 1]:
            to = (me_dp + j) % replicas
            copy = remote(
                proj_out[k].at[to],
                proj_in[k].at[me_dp],
                proj_sem,
                (k, to),
                (k, me_dp),
                dp_id(to),
            )
            copy.start()
            sends.append(copy)

    def turn(k):
        for j in range(replicas):
            source = (me_dp + j) % replicas
            if j > 0:
                remote(
                    proj_out[k].at[source],
                    proj_in[k].at[source],
                    proj_sem,
                    (k, source),
                    (k, source),
                    dp_id(source),
                ).wait_recv()
        proj_in[k][me_dp] = proj_out[k][me_dp]
        for e in range(replicas):
            proj[:, e * cols : (e + 1) * cols] = proj_in[k][e].T

    for k, r in pieces:
        pack(k, r)
    for k in range(chunks):
        if k == 0:
            loads[0].wait()
        project(k)
    for load in right_loads + loads[1:]:
        load.wait()
    for k in range(chunks):
        turn(k)
        for e in range(replicas):
            part = slice(e * quarter, (e + 1) * quarter)
            rotated = jnp.dot(proj[...], right[k][:, part], preferred_element_type=jnp.float32)
            if k > 0:
                rotated = rotated + partial[:, part]
            if k < chunks - 1:
                partial[:, part] = rotated
                continue
            first_new = (
                beta_first * first[:, part].astype(jnp.float32) + (1.0 - beta_first) * rotated
            )
            second_new = (
                beta_second * second[:, part].astype(jnp.float32)
                + (1.0 - beta_second) * rotated * rotated
            )
            direction[:, part] = (
                first_new / bias_first / (jnp.sqrt(second_new / bias_second) + epsilon)
            ).astype(jnp.bfloat16)

    for k in range(chunks):
        for j in [*range(2, replicas), 1, 0]:
            to = (me_dp + j) % replicas
            these = right[k][pl.ds(pl.multiple_of(to * cols, LANES), cols), :]
            result = lax.dot_general(
                direction[...], these, (((1,), (1,)), ((), ())), preferred_element_type=jnp.float32
            ).astype(jnp.bfloat16)
            if j == 0:
                back_own[k] = result
            else:
                back_out[k][j - 1][...] = result
                copy = remote(
                    back_out[k][j - 1],
                    back_in[k].at[me_dp],
                    back_sem,
                    (k, to),
                    (k, me_dp),
                    dp_id(to),
                )
                copy.start()
                sends.append(copy)

    for k in range(chunks):
        for j in range(1, replicas):
            source = (me_dp + j) % replicas
            remote(
                back_out[k][j - 1],
                back_in[k].at[source],
                back_sem,
                (k, source),
                (k, source),
                dp_id(source),
            ).wait_recv()
        back_in[k][me_dp] = back_own[k]
        update[k][...] = (
            jnp.dot(
                left[...], back_in[k][...].reshape(width, cols), preferred_element_type=jnp.float32
            )
            .astype(jnp.bfloat16)
            .reshape(group, rows, cols)
        )
        for to in others:
            copy = remote(
                update[k].at[to],
                returned[k].at[me_group],
                return_sem,
                (k, to),
                (k, me_group),
                group_id(to),
            )
            copy.start()
            sends.append(copy)

    for k in range(chunks):
        for source in others:
            remote(
                update[k].at[source],
                returned[k].at[source],
                return_sem,
                (k, source),
                (k, source),
                group_id(source),
            ).wait_recv()
        returned[k][me_group] = update[k][me_group]
        arrived = [returned[k][s] for s in range(group)]
        for b in range(blocks):
            out[b, :, k * cols : (k + 1) * cols] = pick(slots[b], arrived)

    for copy in sends:
        copy.wait_send()


def nest(counts, shape):
    if not counts:
        return pltpu.VMEM(shape, jnp.bfloat16)
    return [nest(counts[1:], shape) for _ in range(counts[0])]


def fused(grad_parts, owner_table, left_basis, right_basis, first_moment, second_moment):
    replicas, halves, owners = (lax.axis_size(a) for a in ("dp", "half", "own"))
    blocks, rows, width = grad_parts.shape[1:]
    quarter = width // replicas
    group = halves * owners
    far = replicas // 2
    chunks = quarter // LANES
    subs = math.gcd(rows // TILE_ROWS, 4)
    cols, sub_rows = quarter // chunks, rows // subs
    sizes = (replicas, halves, owners, blocks, rows, width, chunks, subs)
    bf16, dma = jnp.bfloat16, pltpu.SemaphoreType.DMA
    hbm = pl.BlockSpec(memory_space=pl.ANY)
    return pl.pallas_call(
        functools.partial(step_kernel, sizes),
        out_shape=jax.ShapeDtypeStruct((blocks, rows, quarter), bf16),
        in_specs=[pl.BlockSpec(memory_space=pltpu.SMEM)] + [hbm] * 5,
        out_specs=pl.BlockSpec(memory_space=pltpu.VMEM),
        scratch_shapes=[
            pltpu.VMEM((width, width), bf16),
            nest((chunks,), (replicas * cols, width)),
            pltpu.VMEM((quarter, width), bf16),
            pltpu.VMEM((quarter, width), bf16),
            nest((far, chunks, subs), (blocks, sub_rows, cols)),
            nest((far, chunks, subs), (blocks, sub_rows, cols)),
            nest((far, chunks, subs), (blocks, sub_rows, cols)),
            nest((far - 1, chunks, subs), (blocks, sub_rows, cols)),
            nest((far - 1, chunks, subs), (blocks, sub_rows, cols)),
            nest((chunks, subs), (group, sub_rows, cols)),
            nest((chunks,), (width, cols)),
            pltpu.VMEM((cols, width), bf16),
            nest((chunks,), (replicas, cols, quarter)),
            nest((chunks,), (replicas, cols, quarter)),
            pltpu.VMEM((quarter, replicas * cols), bf16),
            pltpu.VMEM((quarter, width), jnp.float32),
            pltpu.VMEM((quarter, width), bf16),
            nest((chunks, replicas - 1), (quarter, cols)),
            nest((chunks,), (replicas, quarter, cols)),
            nest((chunks,), (group, rows, cols)),
            nest((chunks,), (group, rows, cols)),
            dma((3,)),
            dma((chunks, replicas)),
            dma((far, chunks, subs)),
            dma((far, chunks, subs)),
            dma((2, far, chunks, subs)),
            dma((2, far - 1, chunks, subs)),
            dma((2, chunks, subs, group)),
            dma((2, chunks, replicas)),
            dma((2, chunks, replicas)),
            dma((2, chunks, group)),
        ],
        compiler_params=pltpu.CompilerParams(collective_id=0, has_side_effects=True),
    )(owner_table.reshape(blocks), grad_parts.reshape(blocks, rows, width), left_basis, right_basis, first_moment, second_moment)


def fits_kernel(mesh, rows, width):
    replicas = mesh.shape["dp"]
    return (
        replicas >= 4
        and replicas % 2 == 0
        and rows % TILE_ROWS == 0
        and width % (replicas * LANES) == 0
    )


def route(mesh, *arrays):
    rows = arrays[0].shape[2]
    body = fused if fits_kernel(mesh, rows, arrays[0].shape[3]) else local
    return body(*arrays)


def solution(mesh):
    return jax.shard_map(
        functools.partial(route, mesh),
        mesh=mesh,
        in_specs=(
            P("dp", None, ("half", "own"), None),
            P(),
            P(("half", "own"), None, None),
            P(("half", "own"), None, None),
            P(("half", "own"), "dp", None),
            P(("half", "own"), "dp", None),
        ),
        out_specs=P(None, ("half", "own"), "dp"),
        check_vma=False,
    )
```
